32 devices in a mesh: groups: 2 (over y), seq: 4 (over z), heads: 2 (over x), cfg: 2 (over core).
Axes of the slice: x: 2, y: 2, z: 4, core: 2. Of those that a mesh axis runs over, the one named last changes fastest.
Arguments:
- video_tokens: bfloat16 [2, 8, 1152, 1024], P('cfg', ('groups', 'seq'), 'heads'), parts along dimension 1, may hold values from -6 to 6
- text_tokens: bfloat16 [2, 8, 1152, 128], P('cfg', ('groups', 'seq'), 'heads'), parts along dimension 1, may hold values from -6 to 6
- text_length: int32 [2, 8], P('cfg', ('groups', 'seq')), parts along dimension 1, may hold values from 1 to 128
- guide_numer: int32 [8], P(('groups', 'seq')), parts along dimension 0, may hold values from 2 to 8
- guide_denom: int32 [8], P(('groups', 'seq')), parts along dimension 0, may hold values from 4 to 8
- spatial_gain: bfloat16 [1152], replicated, may hold values from 0.25 to 1.75
- spatial_qkv: bfloat16 [3, 1152, 1152], P(None, 'heads'), may hold values from -0.11785113 to 0.11785113
- spatial_out: bfloat16 [1152, 1152], P('heads'), may hold values from -0.1875 to 0.1875
- temporal_gain: bfloat16 [1152], replicated, may hold values from 0.25 to 1.75
- temporal_qkv: bfloat16 [3, 1152, 1152], P(None, 'heads'), may hold values from -0.11785113 to 0.11785113
- temporal_out: bfloat16 [1152, 1152], P('heads'), may hold values from -0.1875 to 0.1875
Outputs:
- guided: bfloat16 [8, 1152, 1024], P(('groups', 'seq'), ('heads', 'cfg')), parts along dimension 0
The draws below stay inside these ranges and needn't reach their ends.
There are 2 independent parts, one for each index of `groups`. The reference program is written for one: setup_inputs(seed, part) draws one part's arguments, and reference() takes and returns one part's arrays. A program takes and returns all parts, laid end to end along the dimension named above; an argument that names none is the same for every part. Nothing has to cross between parts.
Inputs may be any that keep to these rules, and one draw needn't show every extreme that they name: `text_length`: text tokens at or beyond a frame's length are padding.
All inputs are finite; a program needn't handle non-finite values.
Results may differ from the reference program's by a relative error of at most 0.009.
Values may be sent and summed in bfloat16 or wider, within the bound.
A program may use at most 64 MiB of HBM per device.

```python
import jax
import jax.numpy as jnp
from jax import lax

D = 1152
HEADS = 16
HEAD_DIM = 72
POS = 1024
TXT = 128
FRAMES = 4


def projection_law(key):
    sigma = D ** (-0.5)
    first = jax.random.fold_in(key, 0)
    values = jnp.clip(jax.random.normal(first, (3, D, D), jnp.float32), -4.0, 4.0) * sigma
    return values.astype(jnp.bfloat16)


def draw_spatial_qkv(key, part):
    return projection_law(jax.random.fold_in(key, 11))


def draw_temporal_qkv(key, part):
    return projection_law(jax.random.fold_in(key, 23))


def draw_video_tokens(key, part):
    key = jax.random.fold_in(key, 31)
    first = jax.random.fold_in(key, 0)
    shape = (2, FRAMES, D, POS)
    values = jnp.clip(jax.random.normal(first, shape, jnp.float32), -6.0, 6.0)
    return values.astype(jnp.bfloat16)


def touch_ends(entries, own_key, low, top_value):
    longest = entries.shape.index(max(entries.shape))
    spots = []
    for shift in (0, 1):
        where = [jax.random.randint(jax.random.fold_in(own_key, axis), (), 0, length) for axis, length in enumerate(entries.shape)]
        where[longest] = (where[longest] + shift) % entries.shape[longest]
        spots.append(tuple(where))
    return entries.at[spots[0]].set(low).at[spots[1]].set(top_value)


def level_of(stream_key, shape, cuts, least, largest):
    level, own = 1.0, jax.random.fold_in(stream_key, 6)
    for position, shards_of in cuts:
        steps = jnp.exp(jax.random.uniform(jax.random.fold_in(own, position), (shards_of,), jnp.float32, least / len(cuts), largest / len(cuts)))
        level = level * jnp.repeat(steps, shape[position] // shards_of).reshape([-1 if axis == position else 1 for axis in range(len(shape))])
    return level


def normal_values(stream_key, shape, scale, most, pieces=(), kind=jnp.bfloat16):
    drawn = jax.random.normal(stream_key, shape, jnp.float32) * scale
    if len(pieces) > 0:
        drawn = level_of(stream_key, shape, pieces, -0.22, 0.18) * drawn
    return jnp.clip(drawn, min=-most, max=most).astype(kind)


def setup_inputs(seed: int = 0, part: int = 0) -> dict:
    key_list = jax.random.split(jax.random.key(seed), 12)
    own_keys = jax.random.split(jax.random.fold_in(key_list[11], part), 12)
    video_tokens = draw_video_tokens(jax.random.fold_in(jax.random.fold_in(key_list[11], part), 71), part)
    text_tokens = normal_values(own_keys[1], (2, FRAMES, D, TXT), 1.0, 6.0, ((0, 2), (1, 4), (2, 2)))
    text_length = touch_ends(jax.random.randint(own_keys[2], (2, FRAMES), 1, TXT + 1), jax.random.fold_in(own_keys[2], 1), 1, TXT).astype(jnp.int32)
    guide_numer = touch_ends(jax.random.randint(own_keys[3], (FRAMES,), 2, 9), jax.random.fold_in(own_keys[3], 1), 2, 8).astype(jnp.int32)
    guide_denom = touch_ends(jax.random.randint(own_keys[4], (FRAMES,), 4, 9), jax.random.fold_in(own_keys[4], 1), 4, 8).astype(jnp.int32)
    spatial_gain = jnp.clip(1.0 + 0.15 * jax.random.normal(key_list[5], (D,), jnp.float32), 0.25, 1.75).astype(jnp.bfloat16)
    spatial_qkv = draw_spatial_qkv(jax.random.fold_in(key_list[11], 71), part)
    spatial_out = normal_values(key_list[7], (D, D), D ** -0.5, 0.1875, ((0, 2),))
    temporal_gain = jnp.clip(1.0 + 0.15 * jax.random.normal(key_list[8], (D,), jnp.float32), 0.25, 1.75).astype(jnp.bfloat16)
    temporal_qkv = draw_temporal_qkv(jax.random.fold_in(key_list[11], 71), part)
    temporal_out = normal_values(key_list[10], (D, D), D ** -0.5, 0.1875, ((0, 2),))
    return dict(video_tokens=video_tokens, text_tokens=text_tokens, text_length=text_length, guide_numer=guide_numer, guide_denom=guide_denom, spatial_gain=spatial_gain, spatial_qkv=spatial_qkv, spatial_out=spatial_out, temporal_gain=temporal_gain, temporal_qkv=temporal_qkv, temporal_out=temporal_out)


epsilon = 1e-06

def normed_project(token_rows, gain_vector, weight_matrix):
    values_wide = token_rows.astype(jnp.float32)
    inverse = lax.rsqrt(lax.optimization_barrier(jnp.mean(values_wide * values_wide, axis=-1)) + epsilon)
    scaled = (values_wide * gain_vector.astype(jnp.float32)).astype(jnp.bfloat16)
    product = jnp.dot(scaled, weight_matrix, preferred_element_type=jnp.float32)
    return (product * inverse[:, None]).astype(jnp.bfloat16)

def softmax_rows(scores):
    top_score = lax.optimization_barrier(jnp.max(scores, axis=-1, keepdims=True))
    expons = jnp.exp(scores - top_score)
    return (expons / lax.optimization_barrier(jnp.sum(expons, axis=-1, keepdims=True))).astype(jnp.bfloat16)

def spatial_attend(query_rows, key_rows, value_rows, valid_keys):
    scores = jnp.einsum('qhe,khe->hqk', query_rows.astype(jnp.float32), key_rows.astype(jnp.float32))
    scores = scores * HEAD_DIM ** (-0.5)
    scores = jnp.where(valid_keys[None, None, :], scores, -jnp.inf)
    weights = softmax_rows(scores)
    result = jnp.einsum('hqk,khe->qhe', weights.astype(jnp.float32), value_rows.astype(jnp.float32))
    return result.astype(jnp.bfloat16)

def reference(video_tokens, text_tokens, text_length, guide_numer, guide_denom, spatial_gain, spatial_qkv, spatial_out, temporal_gain, temporal_qkv, temporal_out):
    frames_all = video_tokens.shape[1]
    spatial_cols = jnp.transpose(spatial_qkv, (2, 0, 1)).reshape(D, 3 * D)
    temporal_cols = jnp.transpose(temporal_qkv, (2, 0, 1)).reshape(D, 3 * D)
    spatial_right = jnp.transpose(spatial_out)
    temporal_right = jnp.transpose(temporal_out)
    outputs = []
    for branch in range(2):
        video_rows = jnp.swapaxes(video_tokens[branch], 1, 2)
        text_rows = jnp.swapaxes(text_tokens[branch], 1, 2)

        def frame_step(inputs):
            frame_rows, frame_text, live_count = inputs
            mixed = normed_project(frame_rows, spatial_gain, spatial_cols).reshape(POS, 3, HEADS, HEAD_DIM)
            context = normed_project(frame_text, spatial_gain, spatial_cols).reshape(TXT, 3, HEADS, HEAD_DIM)
            key_rows = jnp.concatenate([mixed[:, 1], context[:, 1]], axis=0)
            value_rows = jnp.concatenate([mixed[:, 2], context[:, 2]], axis=0)
            valid_keys = jnp.concatenate([jnp.ones((POS,), dtype=bool), jnp.arange(TXT, dtype=jnp.int32) < live_count])
            attended = spatial_attend(mixed[:, 0], key_rows, value_rows, valid_keys).reshape(POS, D)
            update = jnp.dot(attended, spatial_right, preferred_element_type=jnp.float32)
            return (frame_rows.astype(jnp.float32) + update).astype(jnp.bfloat16)
        after_spatial = lax.map(frame_step, (video_rows, text_rows, text_length[branch]))
        flat_rows = after_spatial.reshape(frames_all * POS, D)
        mixed_time = normed_project(flat_rows, temporal_gain, temporal_cols).reshape(frames_all, POS, 3, HEADS, HEAD_DIM)
        scores = jnp.einsum('fphe,gphe->phfg', mixed_time[:, :, 0].astype(jnp.float32), mixed_time[:, :, 1].astype(jnp.float32))
        weights = softmax_rows(scores * HEAD_DIM ** (-0.5))
        attended_time = jnp.einsum('phfg,gphe->fphe', weights.astype(jnp.float32), mixed_time[:, :, 2].astype(jnp.float32))
        attended_time = attended_time.astype(jnp.bfloat16).reshape(frames_all * POS, D)
        update_time = jnp.dot(attended_time, temporal_right, preferred_element_type=jnp.float32)
        block_out = (flat_rows.astype(jnp.float32) + update_time).astype(jnp.bfloat16)
        outputs.append(block_out.reshape(frames_all, POS, D).astype(jnp.float32))
    ratio = guide_numer.astype(jnp.float32) / guide_denom.astype(jnp.float32)
    cond_out = outputs[0]
    uncond_out = outputs[1]
    guided_rows = (uncond_out + ratio[:, None, None] * (cond_out - uncond_out)).astype(jnp.bfloat16)
    return jnp.swapaxes(guided_rows, 1, 2)
```

```python
import functools

import jax
import jax.numpy as jnp
from jax import lax
from jax.experimental import pallas as pl
from jax.experimental.pallas import tpu as pltpu
from jax.sharding import PartitionSpec as P

D = 1152
HEAD_DIM = 72
epsilon = 1e-06
FUSED_MESH = {"groups": 2, "seq": 4, "heads": 2, "cfg": 2}


MESH = pl.DeviceIdType.MESH
LOG2E = 1.4426950408889634
MASKED = -1e30


def block_kernel(
    dims,
    len_ref,
    num_ref,
    den_ref,
    video,
    text,
    gains,
    sqkv,
    so,
    tqkv,
    to,
    out,
    tok,
    gb,
    sc,
    pr,
    wsq,
    wso,
    wt,
    wto,
    qh,
    kt,
    vh,
    att32,
    asend,
    attf,
    st,
    trow,
    tp,
    tat,
    give,
    got,
    gsend,
    keep,
    rts,
    obuf,
    lsem,
    wss,
    wrs,
    tss,
    trs,
    ass,
    ars,
    sss,
    srs,
    rss,
    rrs,
    dss,
    drs,
    gss,
    grs,
):
    width, half, pos, txt, hd = dims
    heads = half // hd
    z = lax.axis_index("seq")
    h = lax.axis_index("heads")
    c = lax.axis_index("cfg")
    y = lax.axis_index("groups")
    frames = 4
    span = pos // 2
    chunk = span // frames
    wide = 2 * chunk
    piece = half // frames
    quarter = half // 2
    rows = quarter
    scale = hd ** (-0.5)
    mine = pl.multiple_of(h * half, 16)
    theirs = pl.multiple_of((1 - h) * half, 16)

    def zx(j):
        hi, lo = z // 2, z % 2
        return (1 - hi if j // 2 else hi) * 2 + (1 - lo if j % 2 else lo)

    def remote(src, dst, ss, rs, **where):
        return pltpu.make_async_remote_copy(
            src_ref=src, dst_ref=dst, send_sem=ss, recv_sem=rs,
            device_id={k: v for k, v in where.items()}, device_id_type=MESH,
        )

    barrier = pltpu.get_barrier_semaphore()
    peers = [{"groups": 1 - y}, {"cfg": 1 - c}]
    for j in range(frames):
        for o in range(2):
            if j or o:
                peers.append({"seq": zx(j), "heads": 1 - h if o else h})
    for peer in peers:
        pl.semaphore_signal(barrier, inc=1, device_id=peer, device_id_type=MESH)
    pl.semaphore_wait(barrier, len(peers))

    set_id = 2 * y + c
    tiles = width // 128

    def pieces(s, zp, side):
        at = pl.ds(pl.multiple_of(side * half + zp * piece, 16), piece)
        lo, hi = tiles * s // 4 * 128, tiles * (s + 1) // 4 * 128
        main = wt.at[s, at, :] if s < 3 else wto.at[at, :]
        return main, wso.at[at, lo:hi]

    def own_pieces(s):
        at = pl.ds(pl.multiple_of(z * piece, 16), piece)
        lo, hi = tiles * s // 4 * 128, tiles * (s + 1) // 4 * 128
        main = tqkv.at[s, at, :] if s < 3 else to.at[at, :]
        return main, so.at[at, lo:hi]

    def x_copies(s):
        return [
            remote(src, dst, wss.at[i], wrs.at[s, z, i], heads=1 - h)
            for i, (src, dst) in enumerate(zip(own_pieces(s), pieces(s, z, h)))
        ]

    def spread(s, zp, slot, **where):
        return [
            remote(ref, ref, wss.at[slot + i], wrs.at[s, zp, i], **where)
            for i, ref in enumerate(pieces(s, zp, 1 - h))
        ]

    def z_copies(s, j):
        return spread(s, z, 2 * j, seq=zx(j))

    def y_copies(s, j):
        return spread(s, zx(j), 8 + 2 * j, groups=1 - y)

    def c_copies(s, j, other):
        return spread(s, zx(j), 16 + 8 * other + 2 * j, cfg=1 - c)

    def arrived(s, j):
        for copy in spread(s, zx(j), 0, heads=1 - h):
            copy.wait_recv()

    def each_set(body):
        for s in range(4):
            pl.when(set_id == s)(functools.partial(body, s))

    def start(copies):
        for copy in copies:
            copy.start()

    each_set(lambda s: start(x_copies(s)))

    cuts = [(pos, txt)] + [(i * wide, wide) for i in range(pos // wide)]

    def token_copy(i):
        lo, n = cuts[i]
        src = text if i == 0 else video.at[:, lo : lo + n]
        return remote(
            src, tok.at[pl.ds(mine, half), lo : lo + n], tss.at[i], trs.at[i], heads=1 - h
        )

    for i in range(len(cuts)):
        token_copy(i).start()

    local = [
        pltpu.make_async_copy(text, tok.at[pl.ds(mine, half), pos : pos + txt], lsem.at[0]),
        pltpu.make_async_copy(video, tok.at[pl.ds(mine, half), 0:pos], lsem.at[1]),
        pltpu.make_async_copy(sqkv, wsq, lsem.at[2]),
        pltpu.make_async_copy(so, wso.at[pl.ds(mine, half), :], lsem.at[3]),
        pltpu.make_async_copy(tqkv, wt.at[:, pl.ds(mine, half), :], lsem.at[4]),
        pltpu.make_async_copy(to, wto.at[pl.ds(mine, half), :], lsem.at[5]),
    ]
    start(local)

    ratio = jnp.full((8, 128), num_ref[0], jnp.int32).astype(jnp.float32) / jnp.full(
        (8, 128), den_ref[0], jnp.int32
    ).astype(jnp.float32)
    rts[z] = ratio

    def ratio_copy(j):
        return remote(rts.at[z], rts.at[z], rss.at[j], rrs.at[z], seq=zx(j))

    for i in range(2):
        for t in range(tiles):
            row = gains[i : i + 1, t * 128 : (t + 1) * 128]
            gb[i, t * 128 : (t + 1) * 128, :] = jnp.transpose(jnp.broadcast_to(row, (128, 128)))
    for j in range(1, frames):
        ratio_copy(j).start()
    for j in range(heads):
        qh[j, 80:128, :] = jnp.zeros((48, pos), jnp.bfloat16)

    def normed(value, i, at):
        tokens = value.astype(jnp.float32)
        sc[:, at * 128 : (at + 1) * 128] = (tokens * gb[i]).astype(jnp.bfloat16)
        return lax.rsqrt(jnp.mean(tokens * tokens, axis=0, keepdims=True) + epsilon)

    def spatial_project(i):
        lo, n = cuts[i]
        inverse = jnp.concatenate(
            [normed(tok[:, lo + 128 * t : lo + 128 * (t + 1)], 0, t) for t in range(n // 128)], axis=1
        )

        def step(r, carry):
            at = pl.ds(pl.multiple_of(r * rows, 16), rows)
            product = jnp.dot(wsq[at, :], sc[:, :n], preferred_element_type=jnp.float32)
            factor = jnp.where(r < half // rows, scale * LOG2E, 1.0)
            pr[at, :n] = product * (inverse * factor)
            return carry

        lax.fori_loop(0 if i else half // rows, 3 * half // rows, step, 0)
        first = lax.broadcasted_iota(jnp.int32, (8, n), 0) == 0
        ones = jnp.where(first, 1.0, 0.0)
        blank = jnp.zeros((128 - hd - 8, n), jnp.float32)
        mask = jnp.zeros((8, n), jnp.float32)
        if i == 0:
            dead = lax.broadcasted_iota(jnp.int32, (8, n), 1) >= len_ref[0, 0]
            mask = jnp.where(jnp.logical_and(first, dead), MASKED, 0.0)

        def unpack(j, carry):
            at = pl.multiple_of(j * hd, 8)
            if i:
                q = jnp.concatenate([pr[pl.ds(at, hd), :n], ones], axis=0)
                qh[j, 0 : hd + 8, lo : lo + n] = q.astype(jnp.bfloat16)
            k = jnp.concatenate([pr[pl.ds(half + at, hd), :n], mask, blank], axis=0)
            kt[j, lo : lo + n, :] = jnp.transpose(k).astype(jnp.bfloat16)
            v = jnp.concatenate([pr[pl.ds(2 * half + at, hd), :n], ones], axis=0)
            vh[j, :, lo : lo + n] = v.astype(jnp.bfloat16)
            return carry

        lax.fori_loop(0, heads, unpack, 0)

    def attend(column):
        column = pl.multiple_of(column, 128)

        def step(i, carry):
            for u in range(2):
                j = 2 * i + u
                scores = jnp.dot(
                    kt[j], qh[j, :, pl.ds(column, wide)], preferred_element_type=jnp.float32
                )
                top = jnp.max(scores, axis=0, keepdims=True)
                weights = jnp.exp2(scores - top).astype(jnp.bfloat16)
                mixed = jnp.dot(vh[j], weights, preferred_element_type=jnp.float32)
                att32[pl.ds(pl.multiple_of(j * hd, 8), hd), :] = mixed[:hd] / mixed[hd : hd + 1]
            return carry

        lax.fori_loop(0, heads // 2, step, 0)
        return att32[...].astype(jnp.bfloat16)

    def attended_copy(j):
        k = pl.multiple_of(zx(j) * chunk, 128)
        return remote(
            asend.at[j],
            attf.at[pl.ds(mine, half), pl.ds(k, chunk)],
            ass.at[j],
            ars.at[j],
            heads=1 - h,
        )

    def state_copy(j):
        return remote(st.at[j], trow.at[z], sss.at[j], srs.at[z], seq=zx(j))

    def out_project(j):
        k = pl.multiple_of(zx(j) * chunk, 128)

        def step(r, carry):
            at = pl.ds(pl.multiple_of(r * rows, 16), rows)
            update = jnp.dot(
                wso[at, :], attf[:, pl.ds(k, chunk)], preferred_element_type=jnp.float32
            )
            base = tok[at, pl.ds(pl.multiple_of(h * span + k, 128), chunk)].astype(jnp.float32)
            state = (base + update).astype(jnp.bfloat16)
            if j:
                st[j, at, :] = state
            else:
                trow[z, at, :] = state
            return carry

        lax.fori_loop(0, width // rows, step, 0)
        if j:
            state_copy(j).start()

    def on_x(s):
        arrived(s, 0)
        for j in (3, 2, 1):
            start(z_copies(s, j))
        start(y_copies(s, 0))
        start(c_copies(s, 0, 0))

    def on_z(j, s):
        arrived(s, j)
        start(y_copies(s, j))
        start(c_copies(s, j, 0))

    def on_y(j, s):
        arrived(s ^ 2, j)
        start(c_copies(s ^ 2, j, 1))

    def on_c(s):
        for j in range(frames):
            arrived(s ^ 1, j)
            arrived(s ^ 3, j)

    each_set(on_x)
    local[0].wait()
    local[1].wait()
    local[2].wait()
    for i in range(len(cuts)):
        token_copy(i).wait_recv()
        spatial_project(i)
        if i == 2:
            each_set(functools.partial(on_y, 0))
            each_set(functools.partial(on_z, 1))
        if i == 3:
            each_set(functools.partial(on_z, 2))
            each_set(functools.partial(on_y, 1))

    for pair in (1, 0):
        near = (zx(2 * pair) // 2) * wide
        result = attend((1 - h) * span + near)
        for j in (2 * pair + 1, 2 * pair):
            low = zx(j) % 2
            asend[j] = jnp.where(low == 0, result[:, :chunk], result[:, chunk:])
            attended_copy(j).start()
        attf[pl.ds(mine, half), pl.ds(pl.multiple_of(near, 128), wide)] = attend(h * span + near)
        if pair:
            each_set(functools.partial(on_z, 3))
            each_set(functools.partial(on_y, 2))
            each_set(functools.partial(on_y, 3))
            each_set(on_c)
            for i in range(3, 6):
                local[i].wait()
        for j in (2 * pair + 1, 2 * pair):
            attended_copy(j).wait_recv()
            out_project(j)

    def arrival(j):
        return remote(st.at[j], trow.at[zx(j)], sss.at[j], srs.at[zx(j)], seq=zx(j))

    for a, b in ((0, 1), (2, 3)):
        for j in (a, b):
            if j:
                arrival(j).wait_recv()
        fa, fb = zx(a), zx(b)
        inverse = jnp.concatenate([normed(trow[fa], 1, 0), normed(trow[fb], 1, 1)], axis=1)

        for m in range(3):

            def step(r, carry, m=m):
                at = pl.ds(pl.multiple_of(r * rows, 16), rows)
                to_at = pl.ds(pl.multiple_of(m * width + r * rows, 16), rows)
                product = jnp.dot(wt[m, at, :], sc[...], preferred_element_type=jnp.float32)
                value = (product * inverse).astype(jnp.bfloat16).astype(jnp.float32)
                tp[fa, to_at, :] = value[:, :chunk]
                tp[fb, to_at, :] = value[:, chunk:]
                return carry

            lax.fori_loop(0, width // rows, step, 0)

    def mix(j, carry):
        at = pl.multiple_of(j * hd, 8)
        q = [tp[f, pl.ds(at, hd), :] for f in range(frames)]
        k = [tp[f, pl.ds(width + at, hd), :] for f in range(frames)]
        v = [tp[f, pl.ds(2 * width + at, hd), :] for f in range(frames)]
        for f in range(frames):
            scores = [jnp.sum(q[f] * k[g], axis=0, keepdims=True) * scale for g in range(frames)]
            top = functools.reduce(jnp.maximum, scores)
            expons = [jnp.exp(score - top) for score in scores]
            total = functools.reduce(jnp.add, expons)
            acc = None
            for g in range(frames):
                weight = (expons[g] / total).astype(jnp.bfloat16).astype(jnp.float32)
                acc = weight * v[g] if acc is None else acc + weight * v[g]
            tat[pl.ds(at, hd), f * chunk : (f + 1) * chunk] = acc
        return carry

    lax.fori_loop(0, 2 * heads, mix, 0)
    for j in range(1, frames):
        remote(rts.at[z], rts.at[zx(j)], rss.at[j], rrs.at[zx(j)], seq=zx(j)).wait_recv()

    tatb = attf
    tatb[...] = tat[...].astype(jnp.bfloat16)

    def temporal_block(q):
        at = pl.ds(pl.multiple_of(q * quarter, 16), quarter)
        update = jnp.dot(wto[at, :], tatb[...], preferred_element_type=jnp.float32)
        base = jnp.concatenate([trow[f, at, :] for f in range(frames)], axis=1)
        return (base.astype(jnp.float32) + update).astype(jnp.bfloat16)

    def give_copy(i):
        return remote(give.at[i], got.at[i], dss.at[i], drs.at[i], cfg=1 - c)

    for i in range(2):
        give[i] = temporal_block(2 * i + 1 - c)
        give_copy(i).start()
    for i in range(2):
        keep[i] = temporal_block(2 * i + c)

    home = pl.multiple_of(h * span + z * chunk, 128)

    def return_copy(i, j):
        o = 2 * j + i
        return remote(
            gsend.at[i, j], obuf.at[:, pl.ds(home, chunk)], gss.at[i, j], grs.at[h, z],
            seq=zx(j), heads=i,
        )

    for i in range(2):
        give_copy(i).wait_recv()
        for j in (3, 2, 1, 0):
            f = zx(j)
            at = pl.ds(pl.multiple_of(f * chunk, 128), chunk)
            own = keep[i, :, at].astype(jnp.float32)
            far = got[i, :, at].astype(jnp.float32)
            cond = jnp.where(c == 0, own, far)
            uncond = jnp.where(c == 0, far, own)
            guided = uncond + rts[f, 0:1, :] * (cond - uncond)
            guided = guided.astype(jnp.bfloat16)
            if j:
                gsend[i, j] = guided
                return_copy(i, j).start()
            else:

                @pl.when(h == i)
                def _():
                    obuf[:, pl.ds(home, chunk)] = guided

                @pl.when(h != i)
                def _():
                    gsend[i, 0] = guided
                    return_copy(i, 0).start()

    def incoming(side, j):
        at = pl.ds(pl.multiple_of(side * span + zx(j) * chunk, 128), chunk)
        return remote(
            gsend.at[0, 0], obuf.at[:, at], gss.at[0, 0], grs.at[side, zx(j)], heads=1 - h
        )

    for j in range(frames):
        if j:
            incoming(h, j).wait_recv()
        incoming(1 - h, j).wait_recv()
    final = pltpu.make_async_copy(obuf, out, lsem.at[6])
    final.start()

    def drain(s):
        for copy in x_copies(s):
            copy.wait_send()
        for j in range(frames):
            if j:
                for copy in z_copies(s, j):
                    copy.wait_send()
            for copy in y_copies(s, j) + c_copies(s, j, 0) + c_copies(s ^ 2, j, 1):
                copy.wait_send()

    each_set(drain)
    for i in range(len(cuts)):
        token_copy(i).wait_send()
    for j in range(frames):
        attended_copy(j).wait_send()
        if j:
            state_copy(j).wait_send()
            ratio_copy(j).wait_send()
    for i in range(2):
        give_copy(i).wait_send()
        for j in range(1, frames):
            return_copy(i, j).wait_send()

        @pl.when(h != i)
        def _(i=i):
            return_copy(i, 0).wait_send()

    final.wait()


def shards_fused(
    video_tokens,
    text_tokens,
    text_length,
    guide_numer,
    guide_denom,
    spatial_gain,
    spatial_qkv,
    spatial_out,
    temporal_gain,
    temporal_qkv,
    temporal_out,
):
    video = video_tokens[0, 0]
    text = text_tokens[0, 0]
    half, pos = video.shape
    txt = text.shape[1]
    width = spatial_gain.shape[0]
    heads = half // HEAD_DIM
    span = pos // 2
    chunk = span // 4
    wide = 2 * chunk
    quarter = half // 2
    gains = jnp.stack([spatial_gain, temporal_gain]).astype(jnp.float32)
    bf16, f32 = jnp.bfloat16, jnp.float32
    smem = pl.BlockSpec(memory_space=pltpu.SMEM)
    hbm = pl.BlockSpec(memory_space=pl.ANY)
    vmem = pl.BlockSpec(memory_space=pltpu.VMEM)
    dma = pltpu.SemaphoreType.DMA
    out = pl.pallas_call(
        functools.partial(block_kernel, (width, half, pos, txt, HEAD_DIM)),
        out_shape=jax.ShapeDtypeStruct((quarter, pos), bf16),
        in_specs=[smem] * 3 + [hbm] * 2 + [vmem] + [hbm] * 4,
        out_specs=hbm,
        scratch_shapes=[
            pltpu.VMEM((width, pos + txt), bf16),
            pltpu.VMEM((2, width, 128), f32),
            pltpu.VMEM((width, wide), bf16),
            pltpu.VMEM((3 * half, wide), f32),
            pltpu.VMEM((3 * half, width), bf16),
            pltpu.VMEM((width, width), bf16),
            pltpu.VMEM((3, width, width), bf16),
            pltpu.VMEM((width, width), bf16),
            pltpu.VMEM((heads, 128, pos), bf16),
            pltpu.VMEM((heads, pos + txt, 128), bf16),
            pltpu.VMEM((heads, HEAD_DIM + 8, pos + txt), bf16),
            pltpu.VMEM((half, wide), f32),
            pltpu.VMEM((4, half, chunk), bf16),
            pltpu.VMEM((width, span), bf16),
            pltpu.VMEM((4, width, chunk), bf16),
            pltpu.VMEM((4, width, chunk), bf16),
            pltpu.VMEM((4, 3 * width, chunk), f32),
            pltpu.VMEM((width, span), f32),
            pltpu.VMEM((2, quarter, span), bf16),
            pltpu.VMEM((2, quarter, span), bf16),
            pltpu.VMEM((2, 4, quarter, chunk), bf16),
            pltpu.VMEM((2, quarter, span), bf16),
            pltpu.VMEM((4, 8, 128), f32),
            pltpu.VMEM((quarter, pos), bf16),
            dma((7,)),
            dma((32,)),
            dma((4, 4, 2)),
            dma((1 + pos // wide,)),
            dma((1 + pos // wide,)),
            dma((4,)),
            dma((4,)),
            dma((4,)),
            dma((4,)),
            dma((4,)),
            dma((4,)),
            dma((2,)),
            dma((2,)),
            dma((2, 4)),
            dma((2, 4)),
        ],
        compiler_params=pltpu.CompilerParams(
            collective_id=0, has_side_effects=True, vmem_limit_bytes=62 * 1024 * 1024
        ),
        name="fused_block",
    )(
        text_length,
        guide_numer,
        guide_denom,
        video,
        text,
        gains,
        spatial_qkv.reshape(3 * half, width),
        spatial_out,
        temporal_qkv,
        temporal_out,
    )
    return out[None]


def from_partner(shard, axis, stride):
    return lax.ppermute(shard, axis, [(i, i ^ 1 << stride) for i in range(lax.axis_size(axis))])


def softmax_along(scores, axis):
    top_score = jnp.max(scores, axis=axis, keepdims=True)
    expons = jnp.exp(scores - top_score)
    return (expons / jnp.sum(expons, axis=axis, keepdims=True)).astype(jnp.bfloat16)


def project_piece(piece, gain_vector, weights, parts):
    gain_piece = gain_vector.astype(jnp.float32)
    weight_piece = weights[parts]
    piece_wide = piece.astype(jnp.float32)
    scaled = (piece_wide * gain_piece[None, :, None]).astype(jnp.bfloat16)
    product = jnp.einsum("kod,fdp->fkop", weight_piece, scaled, preferred_element_type=jnp.float32)
    return (product, jnp.sum(piece_wide * piece_wide, axis=1))


def add_mixed(piece, matrix):
    return jnp.einsum("oc,fcp->fop", matrix, piece, preferred_element_type=jnp.float32)


def shards_many(
    video_tokens,
    text_tokens,
    text_length,
    guide_numer,
    guide_denom,
    spatial_gain,
    spatial_qkv,
    spatial_out,
    temporal_gain,
    temporal_qkv,
    temporal_out,
):
    frame_count = video_tokens.shape[1]
    width = video_tokens.shape[2]
    positions = video_tokens.shape[3]
    text_count = text_tokens.shape[3]
    local_heads = width // HEAD_DIM
    frame_tokens = video_tokens[0]
    frame_text = text_tokens[0]
    video_piece = lax.all_gather(frame_tokens, "heads", axis=1, tiled=True)
    text_piece = lax.all_gather(frame_text, "heads", axis=1, tiled=True)
    video_add, video_sq = project_piece(video_piece, spatial_gain, spatial_qkv, slice(0, 3))
    text_add, text_sq = project_piece(text_piece, spatial_gain, spatial_qkv, slice(1, 3))
    mixed = (video_add * lax.rsqrt(video_sq / D + epsilon)[:, None, None, :]).astype(jnp.bfloat16)
    mixed = mixed.reshape(frame_count, 3, local_heads, HEAD_DIM, positions)
    context = (text_add * lax.rsqrt(text_sq / D + epsilon)[:, None, None, :]).astype(jnp.bfloat16)
    context = context.reshape(frame_count, 2, local_heads, HEAD_DIM, text_count)
    key_rows = jnp.concatenate([mixed[:, 1], context[:, 0]], axis=3)
    value_rows = jnp.concatenate([mixed[:, 2], context[:, 1]], axis=3)
    query_all = mixed[:, 0]
    text_valid = jnp.arange(text_count, dtype=jnp.int32)[None, :] < text_length[0][:, None]
    valid_keys = jnp.concatenate(
        [jnp.ones((frame_count, positions), dtype=bool), text_valid], axis=1
    )
    block_rows = min(512, positions)
    block_count = positions // block_rows
    frame_ids = jnp.repeat(jnp.arange(frame_count, dtype=jnp.int32), block_count)
    block_ids = jnp.tile(jnp.arange(block_count, dtype=jnp.int32), frame_count)

    def block_step(inputs):
        frame_id, block_id = inputs
        query_rows = lax.dynamic_slice_in_dim(
            query_all[frame_id], block_id * block_rows, block_rows, 2
        )
        scores = jnp.einsum(
            "hep,hek->hpk", query_rows, key_rows[frame_id], preferred_element_type=jnp.float32
        )
        scores = scores * HEAD_DIM ** (-0.5)
        scores = jnp.where(valid_keys[frame_id][None, None, :], scores, -jnp.inf)
        weights = softmax_along(scores, 2)
        result = jnp.einsum(
            "hpk,hek->hep", weights, value_rows[frame_id], preferred_element_type=jnp.float32
        )
        return result.astype(jnp.bfloat16)

    attended = lax.map(block_step, (frame_ids, block_ids))
    attended = attended.reshape(frame_count, block_count, local_heads, HEAD_DIM, block_rows)
    attended = jnp.transpose(attended, (0, 2, 3, 1, 4)).reshape(frame_count, width, positions)
    update = add_mixed(lax.all_gather(attended, "heads", axis=1, tiled=True), spatial_out)
    after_spatial = (frame_tokens.astype(jnp.float32) + update).astype(jnp.bfloat16)
    own_rows = lax.all_to_all(after_spatial, "seq", split_axis=2, concat_axis=0, tiled=True)
    frames_all = own_rows.shape[0]
    columns = own_rows.shape[2]
    piece_add, piece_sq = project_piece(
        lax.all_gather(own_rows, "heads", axis=1, tiled=True),
        temporal_gain,
        temporal_qkv,
        slice(0, 3),
    )
    mixed_time = (piece_add * lax.rsqrt(piece_sq / D + epsilon)[:, None, None, :]).astype(
        jnp.bfloat16
    )
    mixed_time = mixed_time.reshape(frames_all, 3, local_heads, HEAD_DIM, columns)
    time_scores = jnp.einsum(
        "fhep,ghep->hfgp", mixed_time[:, 0], mixed_time[:, 1], preferred_element_type=jnp.float32
    )
    time_weights = softmax_along(time_scores * HEAD_DIM ** (-0.5), 2)
    attended_time = jnp.einsum(
        "hfgp,ghep->fhep", time_weights, mixed_time[:, 2], preferred_element_type=jnp.float32
    )
    attended_time = attended_time.astype(jnp.bfloat16).reshape(frames_all, width, columns)
    update_time = add_mixed(
        lax.all_gather(attended_time, "heads", axis=1, tiled=True), temporal_out
    )
    block_out = (own_rows.astype(jnp.float32) + update_time).astype(jnp.bfloat16)
    returned = lax.all_to_all(block_out, "seq", split_axis=0, concat_axis=2, tiled=True)
    half_width = width // 2
    partner = from_partner(returned, "cfg", 0)
    branch_index = lax.axis_index("cfg")
    cond_full = jnp.where(branch_index == 0, returned, partner)
    uncond_full = jnp.where(branch_index == 0, partner, returned)
    cond_part = lax.dynamic_slice_in_dim(cond_full, branch_index * half_width, half_width, 1)
    uncond_part = lax.dynamic_slice_in_dim(uncond_full, branch_index * half_width, half_width, 1)
    ratio = guide_numer.astype(jnp.float32) / guide_denom.astype(jnp.float32)
    cond_wide = cond_part.astype(jnp.float32)
    uncond_wide = uncond_part.astype(jnp.float32)
    return (uncond_wide + ratio[:, None, None] * (cond_wide - uncond_wide)).astype(jnp.bfloat16)


def solution(mesh):
    return jax.shard_map(
        shards_fused if dict(mesh.shape) == FUSED_MESH else shards_many,
        mesh=mesh,
        in_specs=(
            P("cfg", ("groups", "seq"), "heads", None),
            P("cfg", ("groups", "seq"), "heads", None),
            P("cfg", ("groups", "seq")),
            P(("groups", "seq")),
            P(("groups", "seq")),
            P(),
            P(None, "heads", None),
            P("heads", None),
            P(),
            P(None, "heads", None),
            P("heads", None),
        ),
        out_specs=P(("groups", "seq"), ("heads", "cfg"), None),
        check_vma=False,
    )
```

```python
import functools

import jax
import jax.numpy as jnp
from jax import lax
from jax.experimental import pallas as pl
from jax.experimental.pallas import tpu as pltpu
from jax.sharding import PartitionSpec as P

D = 1152
HEAD_DIM = 72
epsilon = 1e-06
FUSED_MESH = {"groups": 2, "seq": 4, "heads": 2, "cfg": 2}


MESH = pl.DeviceIdType.MESH
LOG2E = 1.4426950408889634
MASKED = -1e30


def block_kernel(
    dims,
    len_ref,
    num_ref,
    den_ref,
    video,
    text,
    sgain,
    tgain,
    sqkv,
    so,
    tqkv,
    to,
    obuf,
    tok,
    gb,
    sc,
    pr,
    wsq,
    wso,
    wt,
    wto,
    qh,
    kt,
    vh,
    att32,
    asend,
    attf,
    st,
    trow,
    tp,
    tat,
    give,
    got,
    gsend,
    keep,
    rts,
    sref,
    pref,
    lsem,
    lss,
    lrs,
    wss,
    wrs,
    tss,
    trs,
    ass,
    ars,
    sss,
    srs,
    rss,
    rrs,
    dss,
    drs,
    gss,
    grs,
):
    width, half, pos, txt, hd = dims
    heads = half // hd
    z = lax.axis_index("seq")
    h = lax.axis_index("heads")
    c = lax.axis_index("cfg")
    y = lax.axis_index("groups")
    frames = 4
    span = pos // 2
    chunk = span // frames
    wide = 2 * chunk
    piece = half // frames
    quarter = half // 2
    scale = hd ** (-0.5)
    mine = pl.multiple_of(h * half, 16)
    theirs = pl.multiple_of((1 - h) * half, 16)

    def zx(j):
        hi, lo = z // 2, z % 2
        return (1 - hi if j // 2 else hi) * 2 + (1 - lo if j % 2 else lo)

    def remote(src, dst, ss, rs, **where):
        return pltpu.make_async_remote_copy(
            src_ref=src, dst_ref=dst, send_sem=ss, recv_sem=rs,
            device_id={k: v for k, v in where.items()}, device_id_type=MESH,
        )

    barrier = pltpu.get_barrier_semaphore()
    peers = [{"groups": 1 - y}, {"cfg": 1 - c}]
    for j in range(frames):
        for o in range(2):
            if j or o:
                peers.append({"seq": zx(j), "heads": 1 - h if o else h})
    for peer in peers:
        pl.semaphore_signal(barrier, inc=1, device_id=peer, device_id_type=MESH)
    pl.semaphore_wait(barrier, len(peers))

    set_id = 2 * y + c
    tiles = width // 128

    def columns(s):
        low, high = [tiles * i // 4 * 128 for i in (s, s + 1)]
        return slice(low, high), slice(width - high, width - low)

    def pieces(s, zp, side):
        at = pl.ds(pl.multiple_of(side * half + zp * piece, 16), piece)
        first, second = columns(s)
        return wso.at[at, first], wt.at[0, at, second]

    def own_pieces(s):
        at = pl.ds(pl.multiple_of(z * piece, 16), piece)
        first, second = columns(s)
        return so.at[at, first], tqkv.at[0, at, second]

    def x_copies(s):
        return [
            remote(src, dst, wss.at[i], wrs.at[s, z, i], heads=1 - h)
            for i, (src, dst) in enumerate(zip(own_pieces(s), pieces(s, z, h)))
        ]

    def spread(s, zp, slot, **where):
        return [
            remote(ref, ref, wss.at[slot + i], wrs.at[s, zp, i], **where)
            for i, ref in enumerate(pieces(s, zp, 1 - h))
        ]

    def z_copies(s, j):
        return spread(s, z, 2 * j, seq=zx(j))

    def y_copies(s, j):
        return spread(s, zx(j), 8 + 2 * j, groups=1 - y)

    def c_copies(s, j, other):
        return spread(s, zx(j), 16 + 8 * other + 2 * j, cfg=1 - c)

    def arrived(s, j):
        for copy in spread(s, zx(j), 0, heads=1 - h):
            copy.wait_recv()

    def each_set(body):
        for s in range(4):
            pl.when(set_id == s)(functools.partial(body, s))

    def start(copies):
        for copy in copies:
            copy.start()

    def late(m, side, part):
        at = pl.ds(pl.multiple_of(side * half + part * piece, 16), piece)
        return wt.at[1 + m, at, :] if m < 2 else wto.at[at, :]

    def late_copy(m, slot, part, **where):
        ref = late(m, 1 - h, part)
        return remote(ref, ref, lss.at[m, slot], lrs.at[m, part], **where)

    def late_x(m):
        at = pl.ds(pl.multiple_of(set_id * piece, 16), piece)
        src = tqkv.at[1 + m, at, :] if m < 2 else to.at[at, :]
        return remote(src, late(m, h, set_id), lss.at[m, 0], lrs.at[m, set_id], heads=1 - h)

    across = 2 * (1 - y) + c

    def late_y(m):
        return late_copy(m, 1, set_id, groups=1 - y)

    def late_c(m, other):
        return late_copy(m, 2 + other, across if other else set_id, cfg=1 - c)

    def late_arrived(m, part):
        late_copy(m, 0, part, heads=1 - h).wait_recv()

    def on_late_x(m):
        late_arrived(m, set_id)
        late_y(m).start()
        late_c(m, 0).start()

    def on_late_y(m):
        late_arrived(m, across)
        late_c(m, 1).start()

    def on_late_c(m):
        late_arrived(m, 2 * y + 1 - c)
        late_arrived(m, 2 * (1 - y) + 1 - c)

    each_set(lambda s: start(x_copies(s)))

    cuts = [(pos, txt)] + [(i * wide, wide) for i in range(pos // wide)]

    def token_copy(i):
        lo, n = cuts[i]
        src = text if i == 0 else video.at[:, lo : lo + n]
        return remote(
            src, tok.at[pl.ds(mine, half), lo : lo + n], tss.at[i], trs.at[i], heads=1 - h
        )

    for i in range(len(cuts)):
        token_copy(i).start()
    late_x(0).start()

    local = [
        pltpu.make_async_copy(text, tok.at[pl.ds(mine, half), pos : pos + txt], lsem.at[0]),
        pltpu.make_async_copy(video, tok.at[pl.ds(mine, half), 0:pos], lsem.at[1]),
        pltpu.make_async_copy(sqkv, wsq, lsem.at[2]),
        pltpu.make_async_copy(so, wso.at[pl.ds(mine, half), :], lsem.at[3]),
        pltpu.make_async_copy(tqkv, wt.at[:, pl.ds(mine, half), :], lsem.at[4]),
        pltpu.make_async_copy(to, wto.at[pl.ds(mine, half), :], lsem.at[5]),
    ]
    start(local)

    ratio = jnp.full((8, 128), num_ref[0], jnp.int32).astype(jnp.float32) / jnp.full(
        (8, 128), den_ref[0], jnp.int32
    ).astype(jnp.float32)
    rts[z] = ratio

    def ratio_copy(j):
        return remote(rts.at[z], rts.at[z], rss.at[j], rrs.at[z], seq=zx(j))

    for i, gain in enumerate((sgain, tgain)):
        for t in range(tiles):
            row = gain[:, t * 128 : (t + 1) * 128].astype(jnp.float32)
            gb[i, t * 128 : (t + 1) * 128, :] = jnp.transpose(jnp.broadcast_to(row, (128, 128)))
    for j in range(1, frames):
        ratio_copy(j).start()
    for j in range(heads):
        qh[j, 80:128, :] = jnp.zeros((48, pos), jnp.bfloat16)

    def normed(value, i, at):
        tokens = value.astype(jnp.float32)
        sc[:, at * 128 : (at + 1) * 128] = (tokens * gb[i]).astype(jnp.bfloat16)
        return lax.rsqrt(jnp.mean(tokens * tokens, axis=0, keepdims=True) + epsilon)

    def spatial_project(i):
        lo, n = cuts[i]
        inverse = jnp.concatenate(
            [normed(tok[:, lo + 128 * t : lo + 128 * (t + 1)], 0, t) for t in range(n // 128)], axis=1
        )

        low = 0 if i else half
        product = jnp.dot(wsq[low:, :], sc[:, :n], preferred_element_type=jnp.float32)
        if i:
            pr[:half, :n] = product[:half] * (inverse * (scale * LOG2E))
        pr[half:, :n] = product[half - low :] * inverse
        first = lax.broadcasted_iota(jnp.int32, (8, n), 0) == 0
        ones = jnp.where(first, 1.0, 0.0)
        blank = jnp.zeros((128 - hd - 8, n), jnp.float32)
        mask = jnp.zeros((8, n), jnp.float32)
        if i == 0:
            dead = lax.broadcasted_iota(jnp.int32, (8, n), 1) >= len_ref[0, 0]
            mask = jnp.where(jnp.logical_and(first, dead), MASKED, 0.0)

        def unpack(j, carry):
            at = pl.multiple_of(j * hd, 8)
            if i:
                q = jnp.concatenate([pr[pl.ds(at, hd), :n], ones], axis=0)
                qh[j, 0 : hd + 8, lo : lo + n] = q.astype(jnp.bfloat16)
            k = jnp.concatenate([pr[pl.ds(half + at, hd), :n], mask, blank], axis=0)
            kt[j, lo : lo + n, :] = jnp.transpose(k).astype(jnp.bfloat16)
            v = jnp.concatenate([pr[pl.ds(2 * half + at, hd), :n], ones], axis=0)
            vh[j, :, lo : lo + n] = v.astype(jnp.bfloat16)
            return carry

        lax.fori_loop(0, heads, unpack, 0)

    def attend(column):
        column = pl.multiple_of(column, 128)

        keys = pos + txt
        at = pl.ds(column, wide)

        def score(j, b, top):
            block = slice(b * 128, (b + 1) * 128)
            scores = jnp.dot(kt[j, block, :], qh[j, :, at], preferred_element_type=jnp.float32)
            sref[j % 2, block, :] = scores
            for r in range(16):
                part = scores[8 * r : 8 * r + 8]
                top = part if top is None else jnp.maximum(top, part)
            return top

        top = None
        for b in range(keys // 128):
            top = score(0, b, top)
        for j in range(heads):
            peak = jnp.max(top, axis=0, keepdims=True)
            top = None
            for b in range(keys // 128):
                if j + 1 < heads:
                    top = score(j + 1, b, top)
                block = slice(b * 128, (b + 1) * 128)
                pref[j % 2, block, :] = jnp.exp2(sref[j % 2, block, :] - peak).astype(jnp.bfloat16)
            mixed = jnp.dot(vh[j], pref[j % 2], preferred_element_type=jnp.float32)
            att32[j * hd : (j + 1) * hd, :] = mixed[:hd] / mixed[hd : hd + 1]
        return att32[...].astype(jnp.bfloat16)

    def attended_copy(j):
        k = pl.multiple_of(zx(j) * chunk, 128)
        return remote(
            asend.at[j],
            attf.at[pl.ds(mine, half), pl.ds(k, chunk)],
            ass.at[j],
            ars.at[j],
            heads=1 - h,
        )

    def state_copy(j):
        return remote(st.at[j], trow.at[z], sss.at[j], srs.at[z], seq=zx(j))

    def out_project(j):
        k = pl.multiple_of(zx(j) * chunk, 128)

        update = jnp.dot(wso[...], attf[:, pl.ds(k, chunk)], preferred_element_type=jnp.float32)
        base = tok[:, pl.ds(pl.multiple_of(h * span + k, 128), chunk)].astype(jnp.float32)
        state = (base + update).astype(jnp.bfloat16)
        if j:
            st[j] = state
            state_copy(j).start()
        else:
            trow[z] = state

    def on_x(s):
        arrived(s, 0)
        for j in (3, 2, 1):
            start(z_copies(s, j))
        start(y_copies(s, 0))
        start(c_copies(s, 0, 0))

    def on_z(j, s):
        arrived(s, j)
        start(y_copies(s, j))
        start(c_copies(s, j, 0))

    def on_y(j, s):
        arrived(s ^ 2, j)
        start(c_copies(s ^ 2, j, 1))

    def on_c(s):
        for j in range(frames):
            arrived(s ^ 1, j)
            arrived(s ^ 3, j)

    each_set(on_x)
    local[0].wait()
    local[1].wait()
    local[2].wait()
    for i in range(len(cuts)):
        token_copy(i).wait_recv()
        spatial_project(i)
        for event, j in {
            0: [(on_y, 0)],
            1: [(on_z, 1)],
            2: [(on_z, 2), (on_z, 3), (on_y, 1)],
            3: [(on_y, 2)],
        }.get(i, [(on_y, 3)]):
            each_set(functools.partial(event, j))

    for pair in (1, 0):
        near = (zx(2 * pair) // 2) * wide
        result = attend((1 - h) * span + near)
        for j in (2 * pair + 1, 2 * pair):
            low = zx(j) % 2
            asend[j] = jnp.where(low == 0, result[:, :chunk], result[:, chunk:])
            attended_copy(j).start()
        late_x(2 - pair).start()
        attf[pl.ds(mine, half), pl.ds(pl.multiple_of(near, 128), wide)] = attend(h * span + near)
        if pair:
            each_set(on_c)
            on_late_x(0)
            for i in range(3, 6):
                local[i].wait()
        else:
            on_late_x(1)
        for j in (2 * pair + 1, 2 * pair):
            attended_copy(j).wait_recv()
            out_project(j)

    def arrival(j):
        return remote(st.at[j], trow.at[zx(j)], sss.at[j], srs.at[zx(j)], seq=zx(j))

    for a, b in ((0, 1), (2, 3)):
        if a:
            on_late_x(2)
        for j in (a, b):
            if j:
                arrival(j).wait_recv()
        fa, fb = zx(a), zx(b)
        inverse = jnp.concatenate([normed(trow[fa], 1, 0), normed(trow[fb], 1, 1)], axis=1)

        for m in range(3):
            if a == 0 and m:
                on_late_y(m - 1)
                on_late_c(m - 1)
            at = slice(m * width, (m + 1) * width)
            product = jnp.dot(wt[m], sc[...], preferred_element_type=jnp.float32)
            value = (product * inverse).astype(jnp.bfloat16).astype(jnp.float32)
            tp[fa, at, :] = value[:, :chunk]
            tp[fb, at, :] = value[:, chunk:]

    def mix(j, carry):
        at = pl.multiple_of(j * hd, 8)
        q = [tp[f, pl.ds(at, hd), :] for f in range(frames)]
        k = [tp[f, pl.ds(width + at, hd), :] for f in range(frames)]
        v = [tp[f, pl.ds(2 * width + at, hd), :] for f in range(frames)]
        for f in range(frames):
            scores = [jnp.sum(q[f] * k[g], axis=0, keepdims=True) * scale for g in range(frames)]
            top = functools.reduce(jnp.maximum, scores)
            expons = [jnp.exp(score - top) for score in scores]
            total = functools.reduce(jnp.add, expons)
            acc = None
            for g in range(frames):
                weight = (expons[g] / total).astype(jnp.bfloat16).astype(jnp.float32)
                acc = weight * v[g] if acc is None else acc + weight * v[g]
            tat[pl.ds(at, hd), f * chunk : (f + 1) * chunk] = acc
        return carry

    lax.fori_loop(0, 2 * heads, mix, 0)
    for j in range(1, frames):
        remote(rts.at[z], rts.at[zx(j)], rss.at[j], rrs.at[zx(j)], seq=zx(j)).wait_recv()

    on_late_y(2)
    on_late_c(2)
    tatb = attf
    tatb[...] = tat[...].astype(jnp.bfloat16)

    def temporal_block(q, p):
        at = pl.ds(pl.multiple_of(q * quarter, 16), quarter)
        cols = pl.ds(pl.multiple_of(p * wide, 128), wide)
        update = jnp.dot(wto[at, :], tatb[:, cols], preferred_element_type=jnp.float32)
        base = jnp.concatenate([trow[2 * p + i, at, :] for i in range(2)], axis=1)
        return (base.astype(jnp.float32) + update).astype(jnp.bfloat16)

    def give_copy(i, o):
        return remote(give.at[i, o], got.at[i, o], dss.at[i, o], drs.at[i, o], cfg=1 - c)

    def pair_of(o):
        return z // 2 if o else 1 - z // 2

    def give_pair(o):
        for i in range(2):
            give[i, o] = temporal_block(2 * i + 1 - c, pair_of(o))
            give_copy(i, o).start()

    def keep_pair(o):
        for i in range(2):
            keep[i, o] = temporal_block(2 * i + c, pair_of(o))

    home = pl.multiple_of(h * span + z * chunk, 128)

    def return_copy(i, j):
        o = 2 * j + i
        return remote(
            gsend.at[i, j], obuf.at[:, pl.ds(home, chunk)], gss.at[i, j], grs.at[h, z],
            seq=zx(j), heads=i,
        )

    def guide(o, i):
        give_copy(i, o).wait_recv()
        for j in (1, 0) if o else (3, 2):
            f = zx(j)
            at = pl.ds(pl.multiple_of(f % 2 * chunk, 128), chunk)
            own = keep[i, o, :, at].astype(jnp.float32)
            far = got[i, o, :, at].astype(jnp.float32)
            cond = jnp.where(c == 0, own, far)
            uncond = jnp.where(c == 0, far, own)
            guided = uncond + rts[f, 0:1, :] * (cond - uncond)
            guided = guided.astype(jnp.bfloat16)
            if j:
                gsend[i, j] = guided
                return_copy(i, j).start()
            else:

                @pl.when(h == i)
                def _():
                    obuf[:, pl.ds(home, chunk)] = guided

                @pl.when(h != i)
                def _():
                    gsend[i, 0] = guided
                    return_copy(i, 0).start()

    give_pair(0)
    keep_pair(0)
    give_pair(1)
    for i in range(2):
        guide(0, i)
    keep_pair(1)
    for i in range(2):
        guide(1, i)

    def incoming(side, j):
        at = pl.ds(pl.multiple_of(side * span + zx(j) * chunk, 128), chunk)
        return remote(
            gsend.at[0, 0], obuf.at[:, at], gss.at[0, 0], grs.at[side, zx(j)], heads=1 - h
        )

    for j in range(frames):
        if j:
            incoming(h, j).wait_recv()
        incoming(1 - h, j).wait_recv()
    def drain(s):
        for copy in x_copies(s):
            copy.wait_send()
        for j in range(frames):
            if j:
                for copy in z_copies(s, j):
                    copy.wait_send()
            for copy in y_copies(s, j) + c_copies(s, j, 0) + c_copies(s ^ 2, j, 1):
                copy.wait_send()

    each_set(drain)
    for i in range(len(cuts)):
        token_copy(i).wait_send()
    for j in range(frames):
        attended_copy(j).wait_send()
        if j:
            state_copy(j).wait_send()
            ratio_copy(j).wait_send()
    for i in range(2):
        for o in range(2):
            give_copy(i, o).wait_send()
        for j in range(1, frames):
            return_copy(i, j).wait_send()

        @pl.when(h != i)
        def _(i=i):
            return_copy(i, 0).wait_send()
    for m in range(3):
        late_x(m).wait_send()
        late_y(m).wait_send()
        late_c(m, 0).wait_send()
        late_c(m, 1).wait_send()


def shards_fused(
    video_tokens,
    text_tokens,
    text_length,
    guide_numer,
    guide_denom,
    spatial_gain,
    spatial_qkv,
    spatial_out,
    temporal_gain,
    temporal_qkv,
    temporal_out,
):
    video = video_tokens[0, 0]
    text = text_tokens[0, 0]
    half, pos = video.shape
    txt = text.shape[1]
    width = spatial_gain.shape[0]
    heads = half // HEAD_DIM
    span = pos // 2
    chunk = span // 4
    wide = 2 * chunk
    quarter = half // 2
    bf16, f32 = jnp.bfloat16, jnp.float32
    smem = pl.BlockSpec(memory_space=pltpu.SMEM)
    hbm = pl.BlockSpec(memory_space=pl.ANY)
    vmem = pl.BlockSpec(memory_space=pltpu.VMEM)
    dma = pltpu.SemaphoreType.DMA
    out = pl.pallas_call(
        functools.partial(block_kernel, (width, half, pos, txt, HEAD_DIM)),
        out_shape=jax.ShapeDtypeStruct((quarter, pos), bf16),
        in_specs=[smem] * 3 + [hbm] * 2 + [vmem] * 2 + [hbm] * 4,
        out_specs=vmem,
        scratch_shapes=[
            pltpu.VMEM((width, pos + txt), bf16),
            pltpu.VMEM((2, width, 128), f32),
            pltpu.VMEM((width, wide), bf16),
            pltpu.VMEM((3 * half, wide), f32),
            pltpu.VMEM((3 * half, width), bf16),
            pltpu.VMEM((width, width), bf16),
            pltpu.VMEM((3, width, width), bf16),
            pltpu.VMEM((width, width), bf16),
            pltpu.VMEM((heads, 128, pos), bf16),
            pltpu.VMEM((heads, pos + txt, 128), bf16),
            pltpu.VMEM((heads, HEAD_DIM + 8, pos + txt), bf16),
            pltpu.VMEM((half, wide), f32),
            pltpu.VMEM((4, half, chunk), bf16),
            pltpu.VMEM((width, span), bf16),
            pltpu.VMEM((4, width, chunk), bf16),
            pltpu.VMEM((4, width, chunk), bf16),
            pltpu.VMEM((4, 3 * width, chunk), f32),
            pltpu.VMEM((width, span), f32),
            pltpu.VMEM((2, 2, quarter, wide), bf16),
            pltpu.VMEM((2, 2, quarter, wide), bf16),
            pltpu.VMEM((2, 4, quarter, chunk), bf16),
            pltpu.VMEM((2, 2, quarter, wide), bf16),
            pltpu.VMEM((4, 8, 128), f32),
            pltpu.VMEM((2, pos + txt, wide), f32),
            pltpu.VMEM((2, pos + txt, wide), bf16),
            dma((6,)),
            dma((3, 4)),
            dma((3, 4)),
            dma((32,)),
            dma((4, 4, 2)),
            dma((1 + pos // wide,)),
            dma((1 + pos // wide,)),
            dma((4,)),
            dma((4,)),
            dma((4,)),
            dma((4,)),
            dma((4,)),
            dma((4,)),
            dma((2, 2)),
            dma((2, 2)),
            dma((2, 4)),
            dma((2, 4)),
        ],
        compiler_params=pltpu.CompilerParams(
            collective_id=0, has_side_effects=True, vmem_limit_bytes=62 * 1024 * 1024
        ),
        name="fused_block",
    )(
        text_length,
        guide_numer,
        guide_denom,
        video,
        text,
        spatial_gain.reshape(1, width),
        temporal_gain.reshape(1, width),
        spatial_qkv.reshape(3 * half, width),
        spatial_out,
        temporal_qkv,
        temporal_out,
    )
    return out[None]


def from_partner(shard, axis, stride):
    return lax.ppermute(shard, axis, [(i, i ^ 1 << stride) for i in range(lax.axis_size(axis))])


def softmax_along(scores, axis):
    top_score = jnp.max(scores, axis=axis, keepdims=True)
    expons = jnp.exp(scores - top_score)
    return (expons / jnp.sum(expons, axis=axis, keepdims=True)).astype(jnp.bfloat16)


def project_piece(piece, gain_vector, weights, parts):
    gain_piece = gain_vector.astype(jnp.float32)
    weight_piece = weights[parts]
    piece_wide = piece.astype(jnp.float32)
    scaled = (piece_wide * gain_piece[None, :, None]).astype(jnp.bfloat16)
    product = jnp.einsum("kod,fdp->fkop", weight_piece, scaled, preferred_element_type=jnp.float32)
    return (product, jnp.sum(piece_wide * piece_wide, axis=1))


def add_mixed(piece, matrix):
    return jnp.einsum("oc,fcp->fop", matrix, piece, preferred_element_type=jnp.float32)


def shards_many(
    video_tokens,
    text_tokens,
    text_length,
    guide_numer,
    guide_denom,
    spatial_gain,
    spatial_qkv,
    spatial_out,
    temporal_gain,
    temporal_qkv,
    temporal_out,
):
    frame_count = video_tokens.shape[1]
    width = video_tokens.shape[2]
    positions = video_tokens.shape[3]
    text_count = text_tokens.shape[3]
    local_heads = width // HEAD_DIM
    frame_tokens = video_tokens[0]
    frame_text = text_tokens[0]
    video_piece = lax.all_gather(frame_tokens, "heads", axis=1, tiled=True)
    text_piece = lax.all_gather(frame_text, "heads", axis=1, tiled=True)
    video_add, video_sq = project_piece(video_piece, spatial_gain, spatial_qkv, slice(0, 3))
    text_add, text_sq = project_piece(text_piece, spatial_gain, spatial_qkv, slice(1, 3))
    mixed = (video_add * lax.rsqrt(video_sq / D + epsilon)[:, None, None, :]).astype(jnp.bfloat16)
    mixed = mixed.reshape(frame_count, 3, local_heads, HEAD_DIM, positions)
    context = (text_add * lax.rsqrt(text_sq / D + epsilon)[:, None, None, :]).astype(jnp.bfloat16)
    context = context.reshape(frame_count, 2, local_heads, HEAD_DIM, text_count)
    key_rows = jnp.concatenate([mixed[:, 1], context[:, 0]], axis=3)
    value_rows = jnp.concatenate([mixed[:, 2], context[:, 1]], axis=3)
    query_all = mixed[:, 0]
    text_valid = jnp.arange(text_count, dtype=jnp.int32)[None, :] < text_length[0][:, None]
    valid_keys = jnp.concatenate(
        [jnp.ones((frame_count, positions), dtype=bool), text_valid], axis=1
    )
    block_rows = min(512, positions)
    block_count = positions // block_rows
    frame_ids = jnp.repeat(jnp.arange(frame_count, dtype=jnp.int32), block_count)
    block_ids = jnp.tile(jnp.arange(block_count, dtype=jnp.int32), frame_count)

    def block_step(inputs):
        frame_id, block_id = inputs
        query_rows = lax.dynamic_slice_in_dim(
            query_all[frame_id], block_id * block_rows, block_rows, 2
        )
        scores = jnp.einsum(
            "hep,hek->hpk", query_rows, key_rows[frame_id], preferred_element_type=jnp.float32
        )
        scores = scores * HEAD_DIM ** (-0.5)
        scores = jnp.where(valid_keys[frame_id][None, None, :], scores, -jnp.inf)
        weights = softmax_along(scores, 2)
        result = jnp.einsum(
            "hpk,hek->hep", weights, value_rows[frame_id], preferred_element_type=jnp.float32
        )
        return result.astype(jnp.bfloat16)

    attended = lax.map(block_step, (frame_ids, block_ids))
    attended = attended.reshape(frame_count, block_count, local_heads, HEAD_DIM, block_rows)
    attended = jnp.transpose(attended, (0, 2, 3, 1, 4)).reshape(frame_count, width, positions)
    update = add_mixed(lax.all_gather(attended, "heads", axis=1, tiled=True), spatial_out)
    after_spatial = (frame_tokens.astype(jnp.float32) + update).astype(jnp.bfloat16)
    own_rows = lax.all_to_all(after_spatial, "seq", split_axis=2, concat_axis=0, tiled=True)
    frames_all = own_rows.shape[0]
    columns = own_rows.shape[2]
    piece_add, piece_sq = project_piece(
        lax.all_gather(own_rows, "heads", axis=1, tiled=True),
        temporal_gain,
        temporal_qkv,
        slice(0, 3),
    )
    mixed_time = (piece_add * lax.rsqrt(piece_sq / D + epsilon)[:, None, None, :]).astype(
        jnp.bfloat16
    )
    mixed_time = mixed_time.reshape(frames_all, 3, local_heads, HEAD_DIM, columns)
    time_scores = jnp.einsum(
        "fhep,ghep->hfgp", mixed_time[:, 0], mixed_time[:, 1], preferred_element_type=jnp.float32
    )
    time_weights = softmax_along(time_scores * HEAD_DIM ** (-0.5), 2)
    attended_time = jnp.einsum(
        "hfgp,ghep->fhep", time_weights, mixed_time[:, 2], preferred_element_type=jnp.float32
    )
    attended_time = attended_time.astype(jnp.bfloat16).reshape(frames_all, width, columns)
    update_time = add_mixed(
        lax.all_gather(attended_time, "heads", axis=1, tiled=True), temporal_out
    )
    block_out = (own_rows.astype(jnp.float32) + update_time).astype(jnp.bfloat16)
    returned = lax.all_to_all(block_out, "seq", split_axis=0, concat_axis=2, tiled=True)
    half_width = width // 2
    partner = from_partner(returned, "cfg", 0)
    branch_index = lax.axis_index("cfg")
    cond_full = jnp.where(branch_index == 0, returned, partner)
    uncond_full = jnp.where(branch_index == 0, partner, returned)
    cond_part = lax.dynamic_slice_in_dim(cond_full, branch_index * half_width, half_width, 1)
    uncond_part = lax.dynamic_slice_in_dim(uncond_full, branch_index * half_width, half_width, 1)
    ratio = guide_numer.astype(jnp.float32) / guide_denom.astype(jnp.float32)
    cond_wide = cond_part.astype(jnp.float32)
    uncond_wide = uncond_part.astype(jnp.float32)
    return (uncond_wide + ratio[:, None, None] * (cond_wide - uncond_wide)).astype(jnp.bfloat16)


def solution(mesh):
    return jax.shard_map(
        shards_fused if dict(mesh.shape) == FUSED_MESH else shards_many,
        mesh=mesh,
        in_specs=(
            P("cfg", ("groups", "seq"), "heads", None),
            P("cfg", ("groups", "seq"), "heads", None),
            P("cfg", ("groups", "seq")),
            P(("groups", "seq")),
            P(("groups", "seq")),
            P(),
            P(None, "heads", None),
            P("heads", None),
            P(),
            P(None, "heads", None),
            P("heads", None),
        ),
        out_specs=P(("groups", "seq"), ("heads", "cfg"), None),
        check_vma=False,
    )
```

```python
import functools

import jax
import jax.numpy as jnp
from jax import lax
from jax.experimental import pallas as pl
from jax.experimental.pallas import tpu as pltpu
from jax.sharding import PartitionSpec as P

D = 1152
HEAD_DIM = 72
epsilon = 1e-06
FUSED_MESH = {"groups": 2, "seq": 4, "heads": 2, "cfg": 2}


MESH = pl.DeviceIdType.MESH
LOG2E = 1.4426950408889634
MASKED = -1e30


def block_kernel(
    dims,
    len_ref,
    num_ref,
    den_ref,
    video,
    text,
    sgain,
    tgain,
    sqkv,
    so,
    tqkv,
    to,
    obuf,
    tok,
    gb,
    sc,
    pr,
    wsq,
    wso,
    wt,
    wto,
    qh,
    kt,
    vh,
    att32,
    asend,
    attf,
    st,
    trow,
    tp,
    tat,
    give,
    got,
    gsend,
    keep,
    rts,
    sref,
    pref,
    lsem,
    wss,
    wrs,
    tss,
    trs,
    ass,
    ars,
    sss,
    srs,
    rss,
    rrs,
    dss,
    drs,
    gss,
    grs,
):
    width, half, pos, txt, hd = dims
    heads = half // hd
    z = lax.axis_index("seq")
    h = lax.axis_index("heads")
    c = lax.axis_index("cfg")
    y = lax.axis_index("groups")
    frames = 4
    span = pos // 2
    chunk = span // frames
    wide = 2 * chunk
    piece = half // frames
    quarter = half // 2
    scale = hd ** (-0.5)
    mine = pl.multiple_of(h * half, 16)
    theirs = pl.multiple_of((1 - h) * half, 16)

    def zx(j):
        hi, lo = z // 2, z % 2
        return (1 - hi if j // 2 else hi) * 2 + (1 - lo if j % 2 else lo)

    def remote(src, dst, ss, rs, **where):
        return pltpu.make_async_remote_copy(
            src_ref=src, dst_ref=dst, send_sem=ss, recv_sem=rs,
            device_id={k: v for k, v in where.items()}, device_id_type=MESH,
        )

    barrier = pltpu.get_barrier_semaphore()
    peers = [{"groups": 1 - y}, {"cfg": 1 - c}]
    for j in range(frames):
        for o in range(2):
            if j or o:
                peers.append({"seq": zx(j), "heads": 1 - h if o else h})
    for peer in peers:
        pl.semaphore_signal(barrier, inc=1, device_id=peer, device_id_type=MESH)
    pl.semaphore_wait(barrier, len(peers))

    set_id = 2 * y + c
    tiles = width // 128

    def columns(s, i):
        sizes = [tiles // 4] * 4
        sizes[(3, 0, 1, 2, 0)[i]] += tiles % 4
        return slice(128 * sum(sizes[:s]), 128 * sum(sizes[: s + 1]))

    def pieces(s, zp, side):
        at = pl.ds(pl.multiple_of(side * half + zp * piece, 16), piece)
        main = [wt.at[m, at, columns(s, m + 1)] for m in range(3)]
        return [wso.at[at, columns(s, 0)]] + main + [wto.at[at, columns(s, 4)]]

    def own_pieces(s):
        at = pl.ds(pl.multiple_of(z * piece, 16), piece)
        main = [tqkv.at[m, at, columns(s, m + 1)] for m in range(3)]
        return [so.at[at, columns(s, 0)]] + main + [to.at[at, columns(s, 4)]]

    first, rest, tail, every = (0,), (1, 2, 3), (4,), (0, 1, 2, 3, 4)

    def x_copies(s):
        return [
            remote(src, dst, wss.at[i], wrs.at[s, z, i], heads=1 - h)
            for i, (src, dst) in enumerate(zip(own_pieces(s), pieces(s, z, h)))
        ]

    def spread(group, s, zp, slot, **where):
        refs = pieces(s, zp, 1 - h)
        return [
            remote(refs[i], refs[i], wss.at[slot + i], wrs.at[s, zp, i], **where) for i in group
        ]

    def z_copies(group, s, j):
        return spread(group, s, z, 5 * j, seq=zx(j))

    def y_copies(group, s, j):
        return spread(group, s, zx(j), 20 + 5 * j, groups=1 - y)

    def c_copies(group, s, j, other):
        return spread(group, s, zx(j), 40 + 20 * other + 5 * j, cfg=1 - c)

    def arrived(s, j, group):
        for copy in spread(group, s, zx(j), 0, heads=1 - h):
            copy.wait_recv()

    def each_set(body):
        for s in range(4):
            pl.when(set_id == s)(functools.partial(body, s))

    def start(copies):
        for copy in copies:
            copy.start()

    each_set(lambda s: start(x_copies(s)))

    cuts = [(i * wide, wide) for i in range(pos // wide)] + [(pos, txt)]
    last = len(cuts) - 1

    def token_copy(i):
        lo, n = cuts[i]
        src = text if i == last else video.at[:, lo : lo + n]
        return remote(
            src, tok.at[pl.ds(mine, half), lo : lo + n], tss.at[i], trs.at[i], heads=1 - h
        )

    for i in range(len(cuts)):
        token_copy(i).start()

    local = [
        pltpu.make_async_copy(text, tok.at[pl.ds(mine, half), pos : pos + txt], lsem.at[0]),
        pltpu.make_async_copy(video, tok.at[pl.ds(mine, half), 0:pos], lsem.at[1]),
        pltpu.make_async_copy(sqkv, wsq, lsem.at[2]),
        pltpu.make_async_copy(so, wso.at[pl.ds(mine, half), :], lsem.at[3]),
        pltpu.make_async_copy(tqkv, wt.at[:, pl.ds(mine, half), :], lsem.at[4]),
        pltpu.make_async_copy(to, wto.at[pl.ds(mine, half), :], lsem.at[5]),
    ]
    start(local)

    ratio = jnp.full((8, 128), num_ref[0], jnp.int32).astype(jnp.float32) / jnp.full(
        (8, 128), den_ref[0], jnp.int32
    ).astype(jnp.float32)
    rts[z] = ratio

    def ratio_copy(j):
        return remote(rts.at[z], rts.at[z], rss.at[j], rrs.at[z], seq=zx(j))

    for i, gain in enumerate((sgain, tgain)):
        for t in range(tiles):
            row = gain[t * 128 : (t + 1) * 128].astype(jnp.float32).reshape(1, 128)
            gb[i, t * 128 : (t + 1) * 128, :] = jnp.transpose(jnp.broadcast_to(row, (128, 128)))
    for j in range(1, frames):
        ratio_copy(j).start()
    for j in range(heads):
        qh[j, 80:128, :] = jnp.zeros((48, pos), jnp.bfloat16)

    def normed(value, i, at):
        tokens = value.astype(jnp.float32)
        sc[:, at * 128 : (at + 1) * 128] = (tokens * gb[i]).astype(jnp.bfloat16)
        return lax.rsqrt(jnp.mean(tokens * tokens, axis=0, keepdims=True) + epsilon)

    def spatial_project(i):
        lo, n = cuts[i]
        inverse = jnp.concatenate(
            [normed(tok[:, lo + 128 * t : lo + 128 * (t + 1)], 0, t) for t in range(n // 128)], axis=1
        )

        low = half if i == last else 0
        product = jnp.dot(wsq[low:, :], sc[:, :n], preferred_element_type=jnp.float32)
        if i < last:
            pr[:half, :n] = product[:half] * (inverse * (scale * LOG2E))
        pr[half:, :n] = product[half - low :] * inverse
        first = lax.broadcasted_iota(jnp.int32, (8, n), 0) == 0
        ones = jnp.where(first, 1.0, 0.0)
        blank = jnp.zeros((128 - hd - 8, n), jnp.float32)
        mask = jnp.zeros((8, n), jnp.float32)
        if i == last:
            dead = lax.broadcasted_iota(jnp.int32, (8, n), 1) >= len_ref[0, 0]
            mask = jnp.where(jnp.logical_and(first, dead), MASKED, 0.0)

        def unpack(j, carry):
            at = pl.multiple_of(j * hd, 8)
            if i < last:
                q = jnp.concatenate([pr[pl.ds(at, hd), :n], ones], axis=0)
                qh[j, 0 : hd + 8, lo : lo + n] = q.astype(jnp.bfloat16)
            k = jnp.concatenate([pr[pl.ds(half + at, hd), :n], mask, blank], axis=0)
            kt[j, lo : lo + n, :] = jnp.transpose(k).astype(jnp.bfloat16)
            v = jnp.concatenate([pr[pl.ds(2 * half + at, hd), :n], ones], axis=0)
            vh[j, :, lo : lo + n] = v.astype(jnp.bfloat16)
            return carry

        lax.fori_loop(0, heads, unpack, 0)

    def attend(column):
        column = pl.multiple_of(column, 128)

        keys = pos + txt
        at = pl.ds(column, wide)

        def score(j, b, top):
            block = slice(b * 128, (b + 1) * 128)
            scores = jnp.dot(kt[j, block, :], qh[j, :, at], preferred_element_type=jnp.float32)
            sref[j % 2, block, :] = scores
            for r in range(16):
                part = scores[8 * r : 8 * r + 8]
                top = part if top is None else jnp.maximum(top, part)
            return top

        top = None
        for b in range(keys // 128):
            top = score(0, b, top)
        for j in range(heads):
            peak = jnp.max(top, axis=0, keepdims=True)
            top = None
            for b in range(keys // 128):
                if j + 1 < heads:
                    top = score(j + 1, b, top)
                block = slice(b * 128, (b + 1) * 128)
                pref[j % 2, block, :] = jnp.exp2(sref[j % 2, block, :] - peak).astype(jnp.bfloat16)
            mixed = jnp.dot(vh[j], pref[j % 2], preferred_element_type=jnp.float32)
            att32[j * hd : (j + 1) * hd, :] = mixed[:hd] / mixed[hd : hd + 1]
        return att32[...].astype(jnp.bfloat16)

    def attended_copy(j):
        k = pl.multiple_of(zx(j) * chunk, 128)
        return remote(
            asend.at[j],
            attf.at[pl.ds(mine, half), pl.ds(k, chunk)],
            ass.at[j],
            ars.at[j],
            heads=1 - h,
        )

    def state_copy(j):
        return remote(st.at[j], trow.at[z], sss.at[j], srs.at[z], seq=zx(j))

    def out_project(j):
        k = pl.multiple_of(zx(j) * chunk, 128)

        update = jnp.dot(wso[...], attf[:, pl.ds(k, chunk)], preferred_element_type=jnp.float32)
        base = tok[:, pl.ds(pl.multiple_of(h * span + k, 128), chunk)].astype(jnp.float32)
        state = (base + update).astype(jnp.bfloat16)
        if j:
            st[j] = state
            state_copy(j).start()
        else:
            trow[z] = state

    def on_x(group, s):
        arrived(s, 0, group)
        for j in (3, 2, 1):
            start(z_copies(group, s, j))
        start(y_copies(group, s, 0))
        start(c_copies(group, s, 0, 0))

    def on_z(group, js, s):
        for j in js:
            arrived(s, j, group)
            start(y_copies(group, s, j))
            start(c_copies(group, s, j, 0))

    def on_y(group, js, s):
        for j in js:
            arrived(s ^ 2, j, group)
            start(c_copies(group, s ^ 2, j, 1))

    def on_c(group, s):
        for j in range(frames):
            arrived(s ^ 1, j, group)
            arrived(s ^ 3, j, group)

    def on(event, *args):
        each_set(functools.partial(event, *args))

    on(on_x, first)
    for i in range(3):
        local[i].wait()
    on(on_x, rest)
    on(on_x, tail)
    for i in range(len(cuts)):
        token_copy(i).wait_recv()
        spatial_project(i)
        if i == 0:
            on(on_z, first, (1, 2, 3))
            on(on_y, first, (0,))
        if i == 1:
            on(on_y, first, (1, 2, 3))
        if i == 2:
            on(on_y, rest, (0,))
        if i == 3:
            on(on_z, rest, (1,))

    for pair in (1, 0):
        near = (zx(2 * pair) // 2) * wide

        def side(w, carry, pair=pair, near=near):
            result = attend((1 - h + w * (2 * h - 1)) * span + near)

            @pl.when(w == 0)
            def _():
                for j in (2 * pair + 1, 2 * pair):
                    low = zx(j) % 2
                    asend[j] = jnp.where(low == 0, result[:, :chunk], result[:, chunk:])
                    attended_copy(j).start()

            @pl.when(w == 1)
            def _():
                attf[pl.ds(mine, half), pl.ds(pl.multiple_of(near, 128), wide)] = result

            return carry

        lax.fori_loop(0, 2, side, 0)
        if pair:
            on(on_z, rest, (2, 3))
            on(on_c, first)
            for i in range(3, 6):
                local[i].wait()
        for j in (2 * pair + 1, 2 * pair):
            attended_copy(j).wait_recv()
            out_project(j)
        if pair:
            on(on_y, rest, (1,))
            on(on_z, tail, (1, 2, 3))
    on(on_y, rest, (2, 3))
    on(on_c, rest)
    on(on_y, tail, (0, 1, 2, 3))

    def arrival(j):
        return remote(st.at[j], trow.at[zx(j)], sss.at[j], srs.at[zx(j)], seq=zx(j))

    for a, b in ((0, 1), (2, 3)):
        for j in (a, b):
            if j:
                arrival(j).wait_recv()
        fa, fb = zx(a), zx(b)
        inverse = jnp.concatenate([normed(trow[fa], 1, 0), normed(trow[fb], 1, 1)], axis=1)

        for m in range(3):
            at = slice(m * width, (m + 1) * width)
            product = jnp.dot(wt[m], sc[...], preferred_element_type=jnp.float32)
            value = (product * inverse).astype(jnp.bfloat16).astype(jnp.float32)
            tp[fa, at, :] = value[:, :chunk]
            tp[fb, at, :] = value[:, chunk:]

    def mix(j, carry):
        at = pl.multiple_of(j * hd, 8)
        q = [tp[f, pl.ds(at, hd), :] for f in range(frames)]
        k = [tp[f, pl.ds(width + at, hd), :] for f in range(frames)]
        v = [tp[f, pl.ds(2 * width + at, hd), :] for f in range(frames)]
        for f in range(frames):
            scores = [jnp.sum(q[f] * k[g], axis=0, keepdims=True) * scale for g in range(frames)]
            top = functools.reduce(jnp.maximum, scores)
            expons = [jnp.exp(score - top) for score in scores]
            total = functools.reduce(jnp.add, expons)
            acc = None
            for g in range(frames):
                weight = (expons[g] / total).astype(jnp.bfloat16).astype(jnp.float32)
                acc = weight * v[g] if acc is None else acc + weight * v[g]
            tat[pl.ds(at, hd), f * chunk : (f + 1) * chunk] = acc
        return carry

    lax.fori_loop(0, 2 * heads, mix, 0)
    for j in range(1, frames):
        remote(rts.at[z], rts.at[zx(j)], rss.at[j], rrs.at[zx(j)], seq=zx(j)).wait_recv()

    on(on_c, tail)
    tatb = attf
    tatb[...] = tat[...].astype(jnp.bfloat16)

    def temporal_block(q, p):
        at = pl.ds(pl.multiple_of(q * quarter, 16), quarter)
        cols = pl.ds(pl.multiple_of(p * wide, 128), wide)
        update = jnp.dot(wto[at, :], tatb[:, cols], preferred_element_type=jnp.float32)
        base = jnp.concatenate([trow[2 * p + i, at, :] for i in range(2)], axis=1)
        return (base.astype(jnp.float32) + update).astype(jnp.bfloat16)

    def give_copy(i, o):
        return remote(give.at[i, o], got.at[i, o], dss.at[i, o], drs.at[i, o], cfg=1 - c)

    def pair_of(o):
        return z // 2 if o else 1 - z // 2

    def give_pair(o):
        for i in range(2):
            give[i, o] = temporal_block(2 * i + 1 - c, pair_of(o))
            give_copy(i, o).start()

    def keep_pair(o):
        for i in range(2):
            keep[i, o] = temporal_block(2 * i + c, pair_of(o))

    home = pl.multiple_of(h * span + z * chunk, 128)

    def return_copy(i, j):
        o = 2 * j + i
        return remote(
            gsend.at[i, j], obuf.at[:, pl.ds(home, chunk)], gss.at[i, j], grs.at[h, z],
            seq=zx(j), heads=i,
        )

    def guide(o, i):
        give_copy(i, o).wait_recv()
        for j in (1, 0) if o else (3, 2):
            f = zx(j)
            at = pl.ds(pl.multiple_of(f % 2 * chunk, 128), chunk)
            own = keep[i, o, :, at].astype(jnp.float32)
            far = got[i, o, :, at].astype(jnp.float32)
            cond = jnp.where(c == 0, own, far)
            uncond = jnp.where(c == 0, far, own)
            guided = uncond + rts[f, 0:1, :] * (cond - uncond)
            guided = guided.astype(jnp.bfloat16)
            if j:
                gsend[i, j] = guided
                return_copy(i, j).start()
            else:

                @pl.when(h == i)
                def _():
                    obuf[:, pl.ds(home, chunk)] = guided

                @pl.when(h != i)
                def _():
                    gsend[i, 0] = guided
                    return_copy(i, 0).start()

    give_pair(0)
    keep_pair(0)
    give_pair(1)
    for i in range(2):
        guide(0, i)
    keep_pair(1)
    for i in range(2):
        guide(1, i)

    def incoming(side, j):
        at = pl.ds(pl.multiple_of(side * span + zx(j) * chunk, 128), chunk)
        return remote(
            gsend.at[0, 0], obuf.at[:, at], gss.at[0, 0], grs.at[side, zx(j)], heads=1 - h
        )

    for j in range(frames):
        if j:
            incoming(h, j).wait_recv()
        incoming(1 - h, j).wait_recv()
    def drain(s):
        for copy in x_copies(s):
            copy.wait_send()
        for j in range(frames):
            if j:
                for copy in z_copies(every, s, j):
                    copy.wait_send()
            outgoing = y_copies(every, s, j) + c_copies(every, s, j, 0)
            for copy in outgoing + c_copies(every, s ^ 2, j, 1):
                copy.wait_send()

    each_set(drain)
    for i in range(len(cuts)):
        token_copy(i).wait_send()
    for j in range(frames):
        attended_copy(j).wait_send()
        if j:
            state_copy(j).wait_send()
            ratio_copy(j).wait_send()
    for i in range(2):
        for o in range(2):
            give_copy(i, o).wait_send()
        for j in range(1, frames):
            return_copy(i, j).wait_send()

        @pl.when(h != i)
        def _(i=i):
            return_copy(i, 0).wait_send()


def shards_fused(
    video_tokens,
    text_tokens,
    text_length,
    guide_numer,
    guide_denom,
    spatial_gain,
    spatial_qkv,
    spatial_out,
    temporal_gain,
    temporal_qkv,
    temporal_out,
):
    video = video_tokens[0, 0]
    text = text_tokens[0, 0]
    half, pos = video.shape
    txt = text.shape[1]
    width = spatial_gain.shape[0]
    heads = half // HEAD_DIM
    span = pos // 2
    chunk = span // 4
    wide = 2 * chunk
    quarter = half // 2
    bf16, f32 = jnp.bfloat16, jnp.float32
    smem = pl.BlockSpec(memory_space=pltpu.SMEM)
    hbm = pl.BlockSpec(memory_space=pl.ANY)
    vmem = pl.BlockSpec(memory_space=pltpu.VMEM)
    dma = pltpu.SemaphoreType.DMA
    out = pl.pallas_call(
        functools.partial(block_kernel, (width, half, pos, txt, HEAD_DIM)),
        out_shape=jax.ShapeDtypeStruct((quarter, pos), bf16),
        in_specs=[smem] * 3 + [hbm] * 2 + [vmem] * 2 + [hbm] * 4,
        out_specs=vmem,
        scratch_shapes=[
            pltpu.VMEM((width, pos + txt), bf16),
            pltpu.VMEM((2, width, 128), f32),
            pltpu.VMEM((width, wide), bf16),
            pltpu.VMEM((3 * half, wide), f32),
            pltpu.VMEM((3 * half, width), bf16),
            pltpu.VMEM((width, width), bf16),
            pltpu.VMEM((3, width, width), bf16),
            pltpu.VMEM((width, width), bf16),
            pltpu.VMEM((heads, 128, pos), bf16),
            pltpu.VMEM((heads, pos + txt, 128), bf16),
            pltpu.VMEM((heads, HEAD_DIM + 8, pos + txt), bf16),
            pltpu.VMEM((half, wide), f32),
            pltpu.VMEM((4, half, chunk), bf16),
            pltpu.VMEM((width, span), bf16),
            pltpu.VMEM((4, width, chunk), bf16),
            pltpu.VMEM((4, width, chunk), bf16),
            pltpu.VMEM((4, 3 * width, chunk), f32),
            pltpu.VMEM((width, span), f32),
            pltpu.VMEM((2, 2, quarter, wide), bf16),
            pltpu.VMEM((2, 2, quarter, wide), bf16),
            pltpu.VMEM((2, 4, quarter, chunk), bf16),
            pltpu.VMEM((2, 2, quarter, wide), bf16),
            pltpu.VMEM((4, 8, 128), f32),
            pltpu.VMEM((2, pos + txt, wide), f32),
            pltpu.VMEM((2, pos + txt, wide), bf16),
            dma((6,)),
            dma((80,)),
            dma((4, 4, 5)),
            dma((1 + pos // wide,)),
            dma((1 + pos // wide,)),
            dma((4,)),
            dma((4,)),
            dma((4,)),
            dma((4,)),
            dma((4,)),
            dma((4,)),
            dma((2, 2)),
            dma((2, 2)),
            dma((2, 4)),
            dma((2, 4)),
        ],
        compiler_params=pltpu.CompilerParams(
            collective_id=0, has_side_effects=True, vmem_limit_bytes=62 * 1024 * 1024
        ),
        name="fused_block",
    )(
        text_length,
        guide_numer,
        guide_denom,
        video,
        text,
        spatial_gain,
        temporal_gain,
        spatial_qkv.reshape(3 * half, width),
        spatial_out,
        temporal_qkv,
        temporal_out,
    )
    return out[None]


def from_partner(shard, axis, stride):
    return lax.ppermute(shard, axis, [(i, i ^ 1 << stride) for i in range(lax.axis_size(axis))])


def softmax_along(scores, axis):
    top_score = jnp.max(scores, axis=axis, keepdims=True)
    expons = jnp.exp(scores - top_score)
    return (expons / jnp.sum(expons, axis=axis, keepdims=True)).astype(jnp.bfloat16)


def project_piece(piece, gain_vector, weights, parts):
    gain_piece = gain_vector.astype(jnp.float32)
    weight_piece = weights[parts]
    piece_wide = piece.astype(jnp.float32)
    scaled = (piece_wide * gain_piece[None, :, None]).astype(jnp.bfloat16)
    product = jnp.einsum("kod,fdp->fkop", weight_piece, scaled, preferred_element_type=jnp.float32)
    return (product, jnp.sum(piece_wide * piece_wide, axis=1))


def add_mixed(piece, matrix):
    return jnp.einsum("oc,fcp->fop", matrix, piece, preferred_element_type=jnp.float32)


def shards_many(
    video_tokens,
    text_tokens,
    text_length,
    guide_numer,
    guide_denom,
    spatial_gain,
    spatial_qkv,
    spatial_out,
    temporal_gain,
    temporal_qkv,
    temporal_out,
):
    frame_count = video_tokens.shape[1]
    width = video_tokens.shape[2]
    positions = video_tokens.shape[3]
    text_count = text_tokens.shape[3]
    local_heads = width // HEAD_DIM
    frame_tokens = video_tokens[0]
    frame_text = text_tokens[0]
    video_piece = lax.all_gather(frame_tokens, "heads", axis=1, tiled=True)
    text_piece = lax.all_gather(frame_text, "heads", axis=1, tiled=True)
    video_add, video_sq = project_piece(video_piece, spatial_gain, spatial_qkv, slice(0, 3))
    text_add, text_sq = project_piece(text_piece, spatial_gain, spatial_qkv, slice(1, 3))
    mixed = (video_add * lax.rsqrt(video_sq / D + epsilon)[:, None, None, :]).astype(jnp.bfloat16)
    mixed = mixed.reshape(frame_count, 3, local_heads, HEAD_DIM, positions)
    context = (text_add * lax.rsqrt(text_sq / D + epsilon)[:, None, None, :]).astype(jnp.bfloat16)
    context = context.reshape(frame_count, 2, local_heads, HEAD_DIM, text_count)
    key_rows = jnp.concatenate([mixed[:, 1], context[:, 0]], axis=3)
    value_rows = jnp.concatenate([mixed[:, 2], context[:, 1]], axis=3)
    query_all = mixed[:, 0]
    text_valid = jnp.arange(text_count, dtype=jnp.int32)[None, :] < text_length[0][:, None]
    valid_keys = jnp.concatenate(
        [jnp.ones((frame_count, positions), dtype=bool), text_valid], axis=1
    )
    block_rows = min(512, positions)
    block_count = positions // block_rows
    frame_ids = jnp.repeat(jnp.arange(frame_count, dtype=jnp.int32), block_count)
    block_ids = jnp.tile(jnp.arange(block_count, dtype=jnp.int32), frame_count)

    def block_step(inputs):
        frame_id, block_id = inputs
        query_rows = lax.dynamic_slice_in_dim(
            query_all[frame_id], block_id * block_rows, block_rows, 2
        )
        scores = jnp.einsum(
            "hep,hek->hpk", query_rows, key_rows[frame_id], preferred_element_type=jnp.float32
        )
        scores = scores * HEAD_DIM ** (-0.5)
        scores = jnp.where(valid_keys[frame_id][None, None, :], scores, -jnp.inf)
        weights = softmax_along(scores, 2)
        result = jnp.einsum(
            "hpk,hek->hep", weights, value_rows[frame_id], preferred_element_type=jnp.float32
        )
        return result.astype(jnp.bfloat16)

    attended = lax.map(block_step, (frame_ids, block_ids))
    attended = attended.reshape(frame_count, block_count, local_heads, HEAD_DIM, block_rows)
    attended = jnp.transpose(attended, (0, 2, 3, 1, 4)).reshape(frame_count, width, positions)
    update = add_mixed(lax.all_gather(attended, "heads", axis=1, tiled=True), spatial_out)
    after_spatial = (frame_tokens.astype(jnp.float32) + update).astype(jnp.bfloat16)
    own_rows = lax.all_to_all(after_spatial, "seq", split_axis=2, concat_axis=0, tiled=True)
    frames_all = own_rows.shape[0]
    columns = own_rows.shape[2]
    piece_add, piece_sq = project_piece(
        lax.all_gather(own_rows, "heads", axis=1, tiled=True),
        temporal_gain,
        temporal_qkv,
        slice(0, 3),
    )
    mixed_time = (piece_add * lax.rsqrt(piece_sq / D + epsilon)[:, None, None, :]).astype(
        jnp.bfloat16
    )
    mixed_time = mixed_time.reshape(frames_all, 3, local_heads, HEAD_DIM, columns)
    time_scores = jnp.einsum(
        "fhep,ghep->hfgp", mixed_time[:, 0], mixed_time[:, 1], preferred_element_type=jnp.float32
    )
    time_weights = softmax_along(time_scores * HEAD_DIM ** (-0.5), 2)
    attended_time = jnp.einsum(
        "hfgp,ghep->fhep", time_weights, mixed_time[:, 2], preferred_element_type=jnp.float32
    )
    attended_time = attended_time.astype(jnp.bfloat16).reshape(frames_all, width, columns)
    update_time = add_mixed(
        lax.all_gather(attended_time, "heads", axis=1, tiled=True), temporal_out
    )
    block_out = (own_rows.astype(jnp.float32) + update_time).astype(jnp.bfloat16)
    returned = lax.all_to_all(block_out, "seq", split_axis=0, concat_axis=2, tiled=True)
    half_width = width // 2
    partner = from_partner(returned, "cfg", 0)
    branch_index = lax.axis_index("cfg")
    cond_full = jnp.where(branch_index == 0, returned, partner)
    uncond_full = jnp.where(branch_index == 0, partner, returned)
    cond_part = lax.dynamic_slice_in_dim(cond_full, branch_index * half_width, half_width, 1)
    uncond_part = lax.dynamic_slice_in_dim(uncond_full, branch_index * half_width, half_width, 1)
    ratio = guide_numer.astype(jnp.float32) / guide_denom.astype(jnp.float32)
    cond_wide = cond_part.astype(jnp.float32)
    uncond_wide = uncond_part.astype(jnp.float32)
    return (uncond_wide + ratio[:, None, None] * (cond_wide - uncond_wide)).astype(jnp.bfloat16)


def solution(mesh):
    return jax.shard_map(
        shards_fused if dict(mesh.shape) == FUSED_MESH else shards_many,
        mesh=mesh,
        in_specs=(
            P("cfg", ("groups", "seq"), "heads", None),
            P("cfg", ("groups", "seq"), "heads", None),
            P("cfg", ("groups", "seq")),
            P(("groups", "seq")),
            P(("groups", "seq")),
            P(),
            P(None, "heads", None),
            P("heads", None),
            P(),
            P(None, "heads", None),
            P("heads", None),
        ),
        out_specs=P(("groups", "seq"), ("heads", "cfg"), None),
        check_vma=False,
    )
```
